8 devices in a mesh: dp: 1 (over z), sp: 8 (over y, x, core).
Axes of the slice: x: 2, y: 2, z: 1, core: 2. Of those that a mesh axis runs over, the one named last changes fastest.
Arguments:
- x: bfloat16 [8192, 3072], P(('dp', 'sp'))
- grad_out: bfloat16 [8192, 3072], P(('dp', 'sp'))
- positions: int32 [8192], P(('dp', 'sp'))
- gain: bfloat16 [3072], replicated
- w_q: bfloat16 [3072, 3072], replicated
- w_k: bfloat16 [3072, 1024], replicated
- w_v: bfloat16 [3072, 1024], replicated
- w_o: bfloat16 [3072, 3072], replicated
Outputs:
- output 1: bfloat16 [8192, 3072], P(('dp', 'sp'))
- output 2: bfloat16 [8192, 3072], P(('dp', 'sp'))
- output 3: float32 [3072, 3072], P('dp')
- output 4: float32 [3072, 1024], P('dp')
- output 5: float32 [3072, 1024], P('dp')
- output 6: float32 [3072, 3072], P('dp')
- output 7: float32 [3072], P('dp')
All inputs are finite; a program needn't handle non-finite values.
Results may differ from the reference program's by a relative error of at most 0.02.
Values are sent between devices in bfloat16 or wider.
A program may use at most 1 GiB of HBM per device.

```python
import jax
import jax.numpy as jnp
from jax import lax

D = 3072
HEADS = 24
KV_HEADS = 8
HEAD = 128
SEQ = 8192
GROUP = HEADS // KV_HEADS
ROPE_THETA = 1000000.0
NORM_EPS = 1e-05
NEG_LARGE = -1e30


def block_rows(seq_len, row_cost):
    row_count = seq_len
    while row_count > 8 and row_count * row_cost > 2 ** 24:
        row_count = row_count // 2
    return row_count


def setup_inputs(seed: int = 0, part: int = 0) -> dict:
    base_key = jax.random.key(seed)
    part_key = jax.random.fold_in(base_key, part)
    key_x, key_dy, key_start, key_step = jax.random.split(part_key, 4)
    shared = jax.random.split(jax.random.key(seed + 1), 5)
    x = jax.random.normal(key_x, (SEQ, D), jnp.float32).astype(jnp.bfloat16)
    grad_out = jax.random.normal(key_dy, (SEQ, D), jnp.float32).astype(jnp.bfloat16)
    pos_start = jax.random.randint(key_start, (), 0, SEQ)
    pos_steps = jax.random.randint(key_step, (SEQ,), 1, 4)
    positions = (pos_start + jnp.cumsum(pos_steps) - pos_steps[0]).astype(jnp.int32)
    gain = (1.0 + 0.3 * jax.random.normal(shared[0], (D,), jnp.float32)).astype(jnp.bfloat16)
    w_q = (jax.random.normal(shared[1], (D, HEADS * HEAD), jnp.float32) * D ** -0.5).astype(jnp.bfloat16)
    w_k = (jax.random.normal(shared[2], (D, KV_HEADS * HEAD), jnp.float32) * D ** -0.5).astype(jnp.bfloat16)
    w_v = (jax.random.normal(shared[3], (D, KV_HEADS * HEAD), jnp.float32) * D ** -0.5).astype(jnp.bfloat16)
    w_o = (jax.random.normal(shared[4], (HEADS * HEAD, D), jnp.float32) * (HEADS * HEAD) ** -0.5).astype(jnp.bfloat16)
    return {'x': x, 'grad_out': grad_out, 'positions': positions, 'gain': gain, 'w_q': w_q, 'w_k': w_k, 'w_v': w_v, 'w_o': w_o}


def rope(values, cos_t, sin_t):
    half_dim = HEAD // 2
    lower_half = values[..., :half_dim]
    upper_half = values[..., half_dim:]
    return jnp.concatenate([lower_half * cos_t - upper_half * sin_t, upper_half * cos_t + lower_half * sin_t], axis=-1)


def attend(q_all, k_all, v_all):
    row_count = block_rows(SEQ, HEADS * SEQ)
    n_blocks = SEQ // row_count
    key_f = k_all.astype(jnp.float32)
    val_f = v_all.astype(jnp.float32)
    key_index = jnp.arange(SEQ)
    q_blocks = q_all.reshape(n_blocks, row_count, KV_HEADS, GROUP, HEAD)
    blk_starts = jnp.arange(n_blocks) * row_count

    def one_block(block_args):
        q_blk, blk_start = block_args
        scores = jnp.einsum('qhgd,khd->hgqk', q_blk.astype(jnp.float32), key_f) * HEAD ** -0.5
        causal = (blk_start + jnp.arange(row_count))[:, None] >= key_index[None, :]
        attn_prob = jax.nn.softmax(jnp.where(causal, scores, NEG_LARGE), axis=-1)
        blk_out = jnp.einsum('hgqk,khd->qhgd', attn_prob.astype(jnp.bfloat16).astype(jnp.float32), val_f)
        return blk_out.astype(jnp.bfloat16)

    outputs = lax.map(jax.checkpoint(one_block), (q_blocks, blk_starts))
    return outputs.reshape(SEQ, KV_HEADS, GROUP, HEAD)


def reference(x, grad_out, positions, gain, w_q, w_k, w_v, w_o):
    inv_freq = ROPE_THETA ** (-jnp.arange(0, HEAD, 2).astype(jnp.float32) / HEAD)
    angles = positions.astype(jnp.float32)[:, None] * inv_freq[None, :]
    cos_t = jnp.cos(angles)[:, None, :]
    sin_t = jnp.sin(angles)[:, None, :]

    def forward(x_f, gain_f, wq_f, wk_f, wv_f, wo_f):
        normed = x_f * lax.rsqrt(jnp.mean(x_f * x_f, axis=-1, keepdims=True) + NORM_EPS)
        hidden = (normed * gain_f).astype(jnp.bfloat16).astype(jnp.float32)
        q_proj = jnp.dot(hidden, wq_f, preferred_element_type=jnp.float32).reshape(SEQ, HEADS, HEAD)
        k_proj = jnp.dot(hidden, wk_f, preferred_element_type=jnp.float32).reshape(SEQ, KV_HEADS, HEAD)
        v_all = jnp.dot(hidden, wv_f, preferred_element_type=jnp.float32).astype(jnp.bfloat16).reshape(SEQ, KV_HEADS, HEAD)
        q_all = rope(q_proj, cos_t, sin_t).astype(jnp.bfloat16).reshape(SEQ, KV_HEADS, GROUP, HEAD)
        k_all = rope(k_proj, cos_t, sin_t).astype(jnp.bfloat16)
        attn = attend(q_all, k_all, v_all).reshape(SEQ, HEADS * HEAD)
        mixed = jnp.dot(attn.astype(jnp.float32), wo_f, preferred_element_type=jnp.float32)
        return (x_f + mixed).astype(jnp.bfloat16)

    result, pullback = jax.vjp(forward, x.astype(jnp.float32), gain.astype(jnp.float32), w_q.astype(jnp.float32), w_k.astype(jnp.float32), w_v.astype(jnp.float32), w_o.astype(jnp.float32))
    grad_xf, grad_gain, grad_wq, grad_wk, grad_wv, grad_wo = pullback(grad_out)
    return result, grad_xf.astype(jnp.bfloat16), grad_wq, grad_wk, grad_wv, grad_wo, grad_gain
```

```python
import functools

import jax
import jax.numpy as jnp
from jax import lax
from jax.experimental import pallas as pl
from jax.experimental.pallas import tpu as pltpu
from jax.sharding import PartitionSpec as P


HEAD_DIM = 128
ROPE_THETA = 1000000.0
NORM_EPS = 1e-05
NEG_LARGE = -1e30
LOG2E = 1.4426950408889634
CONTRACT_ROWS = (((0,), (0,)), ((), ()))
CONTRACT_COLS = (((1,), (1,)), ((), ()))
VMEM_LIMIT = 60 * 1024 * 1024
F32 = jnp.float32
BF16 = jnp.bfloat16


def fit(size, want):
    while size % want:
        want //= 2
    return want


def rope_tables(positions):
    inv_freq = ROPE_THETA ** (-jnp.arange(0, HEAD_DIM, 2).astype(F32) / HEAD_DIM)
    angles = positions.astype(F32)[:, None] * inv_freq[None, :]
    cos_t, sin_t = jnp.cos(angles), jnp.sin(angles)
    return jnp.concatenate([cos_t, cos_t], axis=-1), jnp.concatenate([-sin_t, sin_t], axis=-1)


def dot(a, b):
    return jnp.dot(a, b, preferred_element_type=F32)


def dot_nt(a, b):
    return lax.dot_general(a, b, CONTRACT_COLS, preferred_element_type=F32)


def rotate(values, cos_t, sin_t):
    return values * cos_t + pltpu.roll(values, HEAD_DIM // 2, 1) * sin_t


def params(n_axes):
    return pltpu.CompilerParams(dimension_semantics=("arbitrary",) * n_axes, vmem_limit_bytes=VMEM_LIMIT)


def qkv_kernel(group, h_ref, w_ref, cos_ref, sin_ref, q_ref, k_ref, kt_ref, v_ref, vt_ref):
    cos_t, sin_t = cos_ref[...], sin_ref[...]
    proj = dot(h_ref[...], w_ref[...])
    for g in range(group):
        lanes = slice(g * HEAD_DIM, (g + 1) * HEAD_DIM)
        q_ref[:, lanes] = rotate(proj[:, lanes], cos_t, sin_t).astype(BF16)
    key = rotate(proj[:, group * HEAD_DIM:(group + 1) * HEAD_DIM], cos_t, sin_t)
    k_ref[...] = key.astype(BF16)
    kt_ref[...] = key.T.astype(BF16)
    val = proj[:, (group + 1) * HEAD_DIM:]
    v_ref[...] = val.astype(BF16)
    vt_ref[...] = val.T.astype(BF16)


def project(h_all, w_all, cos_t, sin_t, group):
    seq, width = h_all.shape
    rows = fit(seq, 512)
    hd = HEAD_DIM
    return pl.pallas_call(
        functools.partial(qkv_kernel, group),
        grid=(seq // rows,),
        in_specs=[pl.BlockSpec((rows, width), lambda i: (i, 0)),
                  pl.BlockSpec((width, (group + 2) * hd), lambda i: (0, 0)),
                  pl.BlockSpec((rows, hd), lambda i: (i, 0)),
                  pl.BlockSpec((rows, hd), lambda i: (i, 0))],
        out_specs=[pl.BlockSpec((rows, group * hd), lambda i: (i, 0)),
                   pl.BlockSpec((rows, hd), lambda i: (i, 0)),
                   pl.BlockSpec((hd, rows), lambda i: (0, i)),
                   pl.BlockSpec((rows, hd), lambda i: (i, 0)),
                   pl.BlockSpec((hd, rows), lambda i: (0, i))],
        out_shape=[jax.ShapeDtypeStruct((seq, group * hd), BF16),
                   jax.ShapeDtypeStruct((seq, hd), BF16),
                   jax.ShapeDtypeStruct((hd, seq), BF16),
                   jax.ShapeDtypeStruct((seq, hd), BF16),
                   jax.ShapeDtypeStruct((hd, seq), BF16)],
        compiler_params=params(1),
        cost_estimate=pl.CostEstimate(flops=2 * seq * width * (group + 2) * hd, bytes_accessed=2 * seq * width, transcendentals=0),
        name="qkv_proj",
    )(h_all, w_all, cos_t, sin_t)


def do_kernel(group, dy_ref, w_ref, o_ref, do_ref, delta_ref):
    do = dot_nt(dy_ref[...], w_ref[...]).astype(BF16)
    do_ref[...] = do
    prod = do.astype(F32) * o_ref[...].astype(F32)
    for g in range(group):
        delta_ref[g] = jnp.sum(prod[:, g * HEAD_DIM:(g + 1) * HEAD_DIM].T, axis=0, keepdims=True)


def project_do(dy_all, wo_rows, o, group):
    seq, width = dy_all.shape
    rows = fit(seq, 512)
    gw = group * HEAD_DIM
    return pl.pallas_call(
        functools.partial(do_kernel, group),
        grid=(seq // rows,),
        in_specs=[pl.BlockSpec((rows, width), lambda i: (i, 0)),
                  pl.BlockSpec((gw, width), lambda i: (0, 0)),
                  pl.BlockSpec((rows, gw), lambda i: (i, 0))],
        out_specs=[pl.BlockSpec((rows, gw), lambda i: (i, 0)),
                   pl.BlockSpec((group, 1, rows), lambda i: (0, 0, i))],
        out_shape=[jax.ShapeDtypeStruct((seq, gw), BF16),
                   jax.ShapeDtypeStruct((group, 1, seq), F32)],
        compiler_params=params(1),
        cost_estimate=pl.CostEstimate(flops=2 * seq * width * gw, bytes_accessed=2 * seq * width, transcendentals=0),
        name="do_proj",
    )(dy_all, wo_rows, o)


def fwd_kernel(sub, bk, q_ref, k_ref, vt_ref, o_ref, lse_ref, m_ref, l_ref, acc_ref):
    i = pl.program_id(1)
    bq = q_ref.shape[0]
    n_sub = bq // sub
    c = HEAD_DIM ** -0.5 * LOG2E
    m_ref[...] = jnp.full(m_ref.shape, NEG_LARGE, F32)
    l_ref[...] = jnp.zeros(l_ref.shape, F32)
    acc_ref[...] = jnp.zeros(acc_ref.shape, F32)

    def scores(u, k):
        return dot_nt(k, q_ref[u * sub:(u + 1) * sub, :])

    def absorb(u, st, vt):
        cols = slice(u * sub, (u + 1) * sub)
        m_old = m_ref[:, cols]
        m_new = jnp.maximum(m_old, jnp.max(st, axis=0, keepdims=True) * c)
        p = jnp.exp2(st * c - m_new)
        alpha = jnp.exp2(m_old - m_new)
        m_ref[:, cols] = m_new
        l_ref[:, cols] = l_ref[:, cols] * alpha + jnp.sum(p, axis=0, keepdims=True)
        acc_ref[:, cols] = acc_ref[:, cols] * alpha + dot(vt, p.astype(BF16))

    def full_block(j, carry):
        start = pl.multiple_of(j * bk, bk)
        k = k_ref[pl.ds(start, bk), :]
        vt = vt_ref[:, pl.ds(start, bk)]
        st = scores(0, k)
        for u in range(n_sub):
            nxt = scores(u + 1, k) if u + 1 < n_sub else None
            absorb(u, st, vt)
            st = nxt
        return carry

    lax.fori_loop(0, i * (bq // bk), full_block, 0)

    base = pl.multiple_of(i * bq, bq)

    def diag_scores(u):
        rows = (u + 1) * sub
        st = scores(u, k_ref[pl.ds(base, rows), :])
        r = lax.broadcasted_iota(jnp.int32, (rows, sub), 0)
        s = lax.broadcasted_iota(jnp.int32, (rows, sub), 1) + u * sub
        return jnp.where(r <= s, st, NEG_LARGE)

    st = diag_scores(0)
    for u in range(n_sub):
        nxt = diag_scores(u + 1) if u + 1 < n_sub else None
        absorb(u, st, vt_ref[:, pl.ds(base, (u + 1) * sub)])
        st = nxt
    for u in range(n_sub):
        cols = slice(u * sub, (u + 1) * sub)
        l = l_ref[:, cols]
        o_ref[cols, :] = (acc_ref[:, cols] * (1.0 / l)).T.astype(BF16)
        lse_ref[:, cols] = m_ref[:, cols] + jnp.log2(l)


def attention_fwd(q, k, vt, group):
    seq, hd = k.shape
    bq = fit(seq, 1024)
    bk, sub = fit(bq, 512), fit(bq, 256)
    return pl.pallas_call(
        functools.partial(fwd_kernel, sub, bk),
        grid=(group, seq // bq),
        in_specs=[pl.BlockSpec((bq, hd), lambda g, i: (i, g)),
                  pl.BlockSpec((seq, hd), lambda g, i: (0, 0)),
                  pl.BlockSpec((hd, seq), lambda g, i: (0, 0))],
        out_specs=[pl.BlockSpec((bq, hd), lambda g, i: (i, g)),
                   pl.BlockSpec((None, 1, bq), lambda g, i: (g, 0, i))],
        out_shape=[jax.ShapeDtypeStruct((seq, group * hd), BF16),
                   jax.ShapeDtypeStruct((group, 1, seq), F32)],
        scratch_shapes=[pltpu.VMEM((1, bq), F32), pltpu.VMEM((1, bq), F32), pltpu.VMEM((hd, bq), F32)],
        compiler_params=params(2),
        cost_estimate=pl.CostEstimate(flops=2 * group * seq * seq * hd, bytes_accessed=8 * seq * hd * group, transcendentals=group * seq * seq // 2),
        name="attn_fwd",
    )(q, k, vt)


def bwd_kernel(n_prev, half, q_ref, do_ref, k_ref, kt_ref, v_ref, lse_ref, delta_ref, cos_ref, sin_ref, *refs):
    if n_prev:
        dkp_ref, dvp_ref, out_ref, dqt_ref, dk_ref, dv_ref = refs
    else:
        dq_ref, dk_out, dv_out, dqt_ref, dk_ref, dv_ref = refs
    j = pl.program_id(1)
    n = pl.num_programs(1)
    bk = k_ref.shape[0]
    c = HEAD_DIM ** -0.5 * LOG2E

    @pl.when(j == 0)
    def _():
        dqt_ref[...] = jnp.zeros(dqt_ref.shape, F32)

    if n_prev:
        dk_ref[...] = sum(dkp_ref[p] for p in range(n_prev))
        dv_ref[...] = sum(dvp_ref[p] for p in range(n_prev))
    else:
        dk_ref[...] = jnp.zeros(dk_ref.shape, F32)
        dv_ref[...] = jnp.zeros(dv_ref.shape, F32)

    def block(start, width, lo, masked):
        cols = pl.ds(start, width)
        qb, dob = q_ref[cols, :], do_ref[cols, :]
        st = dot_nt(k_ref[lo:, :], qb)
        dpt = dot_nt(v_ref[lo:, :], dob)
        p = jnp.exp2(st * c - lse_ref[:, cols])
        if masked:
            r = lax.broadcasted_iota(jnp.int32, p.shape, 0)
            s = lax.broadcasted_iota(jnp.int32, p.shape, 1)
            p = jnp.where(r <= s, p, 0.0)
        ds = (p * (dpt - delta_ref[:, cols])).astype(BF16)
        pb = p.astype(BF16)
        dv_ref[lo:, :] += dot(pb, dob)
        dk_ref[lo:, :] += dot(ds, qb)
        dqt_ref[:, cols] += dot(kt_ref[:, lo:], ds)

    own = pl.multiple_of(j * bk, bk)
    if half:
        rest = bk - half

        def first_half():
            cols = pl.ds(own, bk)
            qb, dob = q_ref[cols, :], do_ref[cols, :]
            st = dot_nt(k_ref[:half, :], qb)
            dpt = dot_nt(v_ref[:half, :], dob)
            r = lax.broadcasted_iota(jnp.int32, st.shape, 0)
            s = lax.broadcasted_iota(jnp.int32, st.shape, 1)
            p = jnp.where(r <= s, jnp.exp2(st * c - lse_ref[:, cols]), 0.0)
            ds = (p * (dpt - delta_ref[:, cols])).astype(BF16)
            pb = p.astype(BF16)
            dv_ref[:half, :] += dot(pb, dob)
            dk_ref[:half, :] += dot(ds, qb)
            dqt_ref[:, cols] += dot(kt_ref[:, :half], ds)

        first_half()
        block(pl.multiple_of(own + half, half), rest, half, True)
    else:
        block(own, bk, 0, True)

    left = n - 1 - j
    pairs = left // 2

    def pair_body(t, carry):
        start = pl.multiple_of((j + 1 + 2 * t) * bk, bk)
        block(start, 2 * bk, 0, False)
        return carry

    lax.fori_loop(0, pairs, pair_body, 0)

    @pl.when(left % 2 == 1)
    def _():
        block(pl.multiple_of((n - 1) * bk, bk), bk, 0, False)

    scale = HEAD_DIM ** -0.5
    cos_t, sin_t = cos_ref[...], -sin_ref[...]
    dq = rotate(dqt_ref[:, pl.ds(own, bk)].T * scale, cos_t, sin_t).astype(BF16)
    if n_prev:
        hd = HEAD_DIM
        out_ref[:, :hd] = dq
        out_ref[:, hd:2 * hd] = rotate(dk_ref[...] * scale, cos_t, sin_t).astype(BF16)
        out_ref[:, 2 * hd:] = dv_ref[...].astype(BF16)
    else:
        dq_ref[...] = dq
        dk_out[...] = dk_ref[...]
        dv_out[...] = dv_ref[...]


def attention_bwd(first, heads, q, do, k, kt, v, lse, delta, cos_t, sin_t, prev=None):
    seq, hd = k.shape
    bk = fit(seq, 512)
    half = bk // 2 if bk % 256 == 0 else 0
    n_prev = 0 if prev is None else prev[0].shape[0]
    whole = pl.BlockSpec((seq, hd), lambda g, j: (0, first + g))
    row = pl.BlockSpec((None, 1, seq), lambda g, j: (first + g, 0, 0))
    blk = pl.BlockSpec((bk, hd), lambda g, j: (j, 0))
    in_specs = [whole, whole, blk, pl.BlockSpec((hd, bk), lambda g, j: (0, j)), blk, row, row, blk, blk]
    args = [q, do, k, kt, v, lse, delta, cos_t, sin_t]
    if prev is None:
        part = pl.BlockSpec((None, bk, hd), lambda g, j: (g, j, 0))
        out_specs = [pl.BlockSpec((bk, hd), lambda g, j: (j, g)), part, part]
        out_shape = [jax.ShapeDtypeStruct((seq, heads * hd), BF16)] + [jax.ShapeDtypeStruct((heads, seq, hd), F32)] * 2
    else:
        part = pl.BlockSpec((n_prev, bk, hd), lambda g, j: (0, j, 0))
        in_specs += [part, part]
        args += list(prev)
        out_specs = pl.BlockSpec((bk, 3 * hd), lambda g, j: (j, 0))
        out_shape = jax.ShapeDtypeStruct((seq, 3 * hd), BF16)
    return pl.pallas_call(
        functools.partial(bwd_kernel, n_prev, half),
        grid=(heads, seq // bk),
        in_specs=in_specs,
        out_specs=out_specs,
        out_shape=out_shape,
        scratch_shapes=[pltpu.VMEM((hd, seq), F32), pltpu.VMEM((bk, hd), F32), pltpu.VMEM((bk, hd), F32)],
        compiler_params=params(2),
        cost_estimate=pl.CostEstimate(flops=5 * heads * seq * seq * hd, bytes_accessed=16 * seq * hd * heads, transcendentals=heads * seq * seq // 2),
        name="attn_bwd_last" if n_prev else "attn_bwd",
    )(*args)


def assemble_q_kernel(a_ref, b_ref, wq_ref):
    first = a_ref.shape[1]
    wq_ref[:, :first] = a_ref[...]
    wq_ref[:, first:] = b_ref[...]


def assemble_q(early, late):
    parts, rows, first = early.shape
    second = late.shape[2]
    br = fit(rows, 1024)
    return pl.pallas_call(
        assemble_q_kernel,
        grid=(parts, rows // br),
        in_specs=[pl.BlockSpec((None, br, first), lambda s, r: (s, r, 0)),
                  pl.BlockSpec((None, br, second), lambda s, r: (s, r, 0))],
        out_specs=pl.BlockSpec((br, first + second), lambda s, r: (r, s)),
        out_shape=jax.ShapeDtypeStruct((rows, parts * (first + second)), F32),
        compiler_params=params(2),
        cost_estimate=pl.CostEstimate(flops=parts * rows * 1024, bytes_accessed=8 * parts * rows * (first + second), transcendentals=0),
        name="assemble_dwq",
    )(early, late)


def assemble_kv_kernel(a_ref, wk_ref, wv_ref):
    hd = HEAD_DIM
    wk_ref[...] = a_ref[:, :hd]
    wv_ref[...] = a_ref[:, hd:]


def assemble_kv(both):
    parts, rows, _ = both.shape
    hd = HEAD_DIM
    br = fit(rows, 1024)
    out = pl.BlockSpec((br, hd), lambda s, r: (r, s))
    return pl.pallas_call(
        assemble_kv_kernel,
        grid=(parts, rows // br),
        in_specs=[pl.BlockSpec((None, br, 2 * hd), lambda s, r: (s, r, 0))],
        out_specs=[out, out],
        out_shape=[jax.ShapeDtypeStruct((rows, parts * hd), F32)] * 2,
        compiler_params=params(2),
        cost_estimate=pl.CostEstimate(flops=parts * rows * 1024, bytes_accessed=8 * parts * rows * 2 * hd, transcendentals=0),
        name="assemble_dwkv",
    )(both)


def copy_kernel(a_ref, b_ref):
    b_ref[...] = a_ref[...]


def copy_out(a):
    rows, cols = a.shape
    br = fit(rows, 256)
    spec = pl.BlockSpec((br, cols), lambda i: (i, 0))
    return pl.pallas_call(
        copy_kernel, grid=(rows // br,), in_specs=[spec], out_specs=spec,
        out_shape=jax.ShapeDtypeStruct(a.shape, a.dtype), compiler_params=params(1),
        cost_estimate=pl.CostEstimate(flops=rows * 1024, bytes_accessed=8 * rows * cols, transcendentals=0),
        name="copy_dwo",
    )(a)


def solution(mesh):
    sp_size = mesh.shape['sp']
    seq_spec = P(('dp', 'sp'), None)
    pos_spec = P(('dp', 'sp'))
    replicated = P(None, None)
    part_rows = P('dp', None)

    def local_step(x, grad_out, positions, gain, w_q, w_k, w_v, w_o):
        tok, width = x.shape
        hd = HEAD_DIM
        group = w_q.shape[1] // hd // sp_size
        assert w_k.shape[1] // hd == sp_size and group >= 2
        gw = group * hd
        me = lax.axis_index('sp')

        x_f = x.astype(F32)
        inv_rms = lax.rsqrt(jnp.mean(x_f * x_f, axis=-1, keepdims=True) + NORM_EPS)
        normed = x_f * inv_rms
        gain_f = gain.astype(F32)
        hidden = (normed * gain_f).astype(BF16)
        h_all = lax.all_gather(hidden, 'sp', axis=0, tiled=True)

        pos_all = lax.all_gather(positions, 'sp', axis=0, tiled=True)
        cos_t, sin_t = rope_tables(pos_all)
        w_all = jnp.concatenate([lax.dynamic_slice(w_q, (0, me * gw), (width, gw)),
                                 lax.dynamic_slice(w_k, (0, me * hd), (width, hd)),
                                 lax.dynamic_slice(w_v, (0, me * hd), (width, hd))], axis=1)
        wo_rows = lax.dynamic_slice(w_o, (me * gw, 0), (gw, width))

        dy_late, _, cos_t, sin_t, w_all, wo_rows = lax.optimization_barrier((grad_out, hidden, cos_t, sin_t, w_all, wo_rows))
        dy_all = lax.all_gather(dy_late, 'sp', axis=0, tiled=True)

        q, k, kt, v, vt = project(h_all, w_all, cos_t, sin_t, group)
        o, lse = attention_fwd(q, k, vt, group)

        o_loc = lax.all_to_all(o.reshape(sp_size, tok, gw), 'sp', 0, 0, tiled=True)
        wo_block = lax.dot_general(o, dy_all, CONTRACT_ROWS, preferred_element_type=F32)
        grad_wo = lax.all_gather(wo_block, 'sp', axis=0, tiled=True)
        grad_wo = copy_out(grad_wo)
        do, delta = project_do(dy_all, wo_rows, o, group)

        early = group - 1
        dq_a, dk_p, dv_p = attention_bwd(0, early, q, do, k, kt, v, lse, delta, cos_t, sin_t)
        dq_a_loc = lax.all_to_all(dq_a.reshape(sp_size, tok, early * hd), 'sp', 0, 0, tiled=True)
        dw_a = lax.dot_general(h_all, dq_a, CONTRACT_ROWS, preferred_element_type=F32)
        dw_a_all = lax.all_gather(dw_a, 'sp', axis=0)
        d_b = attention_bwd(early, 1, q, do, k, kt, v, lse, delta, cos_t, sin_t, prev=(dk_p, dv_p))
        d_b_loc = lax.all_to_all(d_b.reshape(sp_size, tok, 3 * hd), 'sp', 0, 0, tiled=True)
        dw_b = lax.dot_general(h_all, d_b[:, :hd], CONTRACT_ROWS, preferred_element_type=F32)
        dw_b_all = lax.all_gather(dw_b, 'sp', axis=0)
        dw_c = lax.dot_general(h_all, d_b[:, hd:], CONTRACT_ROWS, preferred_element_type=F32)
        dw_c_all = lax.all_gather(dw_c, 'sp', axis=0)

        o_rows = jnp.transpose(o_loc, (1, 0, 2)).reshape(tok, sp_size * gw)
        result = (x_f + dot(o_rows, w_o)).astype(BF16)

        dq_pre = jnp.transpose(jnp.concatenate([dq_a_loc, d_b_loc[:, :, :hd]], axis=-1), (1, 0, 2)).reshape(tok, sp_size * gw)
        dk_pre = jnp.transpose(d_b_loc[:, :, hd:2 * hd], (1, 0, 2)).reshape(tok, sp_size * hd)
        dv_pre = jnp.transpose(d_b_loc[:, :, 2 * hd:], (1, 0, 2)).reshape(tok, sp_size * hd)
        d_hidden = dot_nt(dq_pre, w_q) + dot_nt(dk_pre, w_k) + dot_nt(dv_pre, w_v)
        grad_gain = lax.psum(jnp.sum(d_hidden * normed, axis=0), 'sp')
        d_normed = d_hidden * gain_f
        d_xnorm = inv_rms * (d_normed - normed * jnp.mean(d_normed * normed, axis=-1, keepdims=True))
        grad_x = (grad_out.astype(F32) + d_xnorm).astype(BF16)

        grad_wq = assemble_q(dw_a_all, dw_b_all)
        grad_wk, grad_wv = assemble_kv(dw_c_all)
        return result, grad_x, grad_wq, grad_wk, grad_wv, grad_wo, grad_gain

    return jax.shard_map(local_step, mesh=mesh,
                         in_specs=(seq_spec, seq_spec, pos_spec, P(None), replicated, replicated, replicated, replicated),
                         out_specs=(seq_spec, seq_spec, part_rows, part_rows, part_rows, part_rows, P('dp')),
                         check_vma=False)
```
